512 devices in a mesh: dp: 2 (over y_lo), ctx: 16 (over y_hi, x, core), tensor: 16 (over z).
Axes of the slice: x: 4, y: 4 (y_hi: 2, y_lo: 2; y = y_hi * 2 + y_lo), z: 16, core: 2. Of those that a mesh axis runs over, the one named last changes fastest.
Arguments:
- residual: bfloat16 [8192, 3584], P(('dp', 'ctx', 'tensor')), parts along dimension 0, may hold values from -6 to 6
- queries: bfloat16 [8192, 4096], P(('dp', 'ctx'), 'tensor'), parts along dimension 0, may hold values from -8 to 8
- key_heads: bfloat16 [8192, 2048], P(('dp', 'ctx'), 'tensor'), parts along dimension 0, may hold values from -8 to 8
- value_heads: bfloat16 [8192, 2048], P(('dp', 'ctx'), 'tensor'), parts along dimension 0, may hold values from -6 to 6
- doc_blocks: int32 [12], P('dp'), parts along dimension 0, may hold values from 1 to 64, 128 in all
- out_weight: bfloat16 [4096, 3584], P('tensor'), may hold values from -0.265625 to 0.265625
- post_gain: float32 [3584], replicated, may hold values from 0.1 to 1.9
- ffn_gain: float32 [3584], replicated, may hold values from 0.1 to 1.9
- gate_weight: bfloat16 [3584, 14336], P('ctx', 'tensor'), may hold values from -0.09375 to 0.09375
- up_weight: bfloat16 [3584, 14336], P('ctx', 'tensor'), may hold values from -0.09375 to 0.09375
Outputs:
- mixed_stream: bfloat16 [8192, 3584], P(('dp', 'ctx', 'tensor')), parts along dimension 0
- ffn_hidden: bfloat16 [8192, 14336], P(('dp', 'ctx'), 'tensor'), parts along dimension 0
The draws below stay inside these ranges and needn't reach their ends.
There are 2 independent parts, one for each index of `dp`. The reference program is written for one: setup_inputs(seed, part) draws one part's arguments, and reference() takes and returns one part's arrays. A program takes and returns all parts, laid end to end along the dimension named above; an argument that names none is the same for every part. Nothing has to cross between parts.
Inputs may be any that keep to these rules, and one draw needn't show every extreme that they name: `doc_blocks`: the lengths, in blocks of 32 positions, of the 6 documents packed in order into the sequence; they sum to 128, and the longest has exactly 64 blocks.
All inputs are finite; a program needn't handle non-finite values.
Results may differ from the reference program's by a relative error of at most 0.025.
Values may be sent and summed in bfloat16 or wider, within the bound.
No kernel may reach another device: no remote copies, remote signals or barrier semaphores. Data moves between devices by JAX's collectives and lax.ppermute only.
A program may use at most 64 MiB of HBM per device.

```python
import math
import jax
import jax.numpy as jnp
import numpy as np
from jax import lax

D = 3584
HD = 256
H = 16
KVH = 8
FF = 14336
TOK_CTX = 256
LENGTH = 4096
BLOCK = 32
NBLK = 128
DOCS = 6
MOST_BLK = 64


def draw_out_weight(key, part):
    fan_rows = H * HD
    drawn = jnp.clip(jax.random.normal(key, (fan_rows, D), jnp.float32), -5.0, 5.0) * fan_rows ** (-0.5)
    return drawn.astype(jnp.bfloat16)


def background(key, array_shape):
    sample = jnp.clip(jax.random.normal(key, array_shape, jnp.float32), -6.0, 6.0)
    return sample


def aligned_plan(key):
    plan_key = jax.random.fold_in(key, 7301)
    block_shape = (NBLK, 1, KVH)
    marked = jax.random.randint(jax.random.fold_in(plan_key, 1), block_shape, 0, 2) == 0
    offset = jax.random.randint(jax.random.fold_in(plan_key, 2), block_shape, 0, BLOCK // 2)
    which_query = jax.random.randint(jax.random.fold_in(plan_key, 3), block_shape, 0, 2)
    own_higher = jax.random.randint(jax.random.fold_in(plan_key, 4), block_shape, 0, 2) == 1
    sign_table = (jax.random.randint(jax.random.fold_in(plan_key, 5), (NBLK, 1, KVH, HD), 0, 2) * 2 - 1).astype(jnp.float32)
    places = jnp.arange(BLOCK, dtype=jnp.int32)[None, :, None]
    own_hit = marked & (places == 2 * offset + 1)
    prev_hit = marked & (places == 2 * offset)
    dim_index = jnp.arange(HD, dtype=jnp.int32)
    slow_dims = (dim_index % (HD // 2) >= HD // 4).astype(jnp.float32)
    pattern = sign_table * slow_dims
    top_score = jax.random.uniform(jax.random.fold_in(plan_key, 6), block_shape, jnp.float32, 68.0, 80.0)
    score_gap = jax.random.uniform(jax.random.fold_in(plan_key, 7), block_shape, jnp.float32, 3.0, 8.0)
    head_root = math.sqrt(HD)
    scale_query = jnp.sqrt(2.0 * top_score / head_root)
    own_score = jnp.where(own_higher, top_score, top_score - score_gap)
    prev_score = jnp.where(own_higher, top_score - score_gap, top_score)
    own_level = own_score / (scale_query * head_root / 2.0)
    prev_level = prev_score / (scale_query * head_root / 2.0)
    return (own_hit, prev_hit, which_query, pattern, slow_dims, scale_query, own_level, prev_level)


def draw_key_heads(key, part):
    own_hit, prev_hit, which_query, pattern, slow_dims, scale_query, own_level, prev_level = aligned_plan(key)
    filler = background(jax.random.fold_in(key, 31), (NBLK, BLOCK, KVH, HD))
    key_level = jnp.where(own_hit, own_level, prev_level)
    aligned = key_level[..., None] * pattern + filler * (1.0 - slow_dims)
    hit_any = own_hit | prev_hit
    values = jnp.where(hit_any[..., None], aligned, filler)
    return values.reshape(LENGTH, KVH * HD).astype(jnp.bfloat16)


def draw_queries(key, part):
    own_hit, prev_hit, which_query, pattern, slow_dims, scale_query, own_level, prev_level = aligned_plan(key)
    filler = background(jax.random.fold_in(key, 37), (NBLK, BLOCK, H, HD))
    head_parity = (jnp.arange(H, dtype=jnp.int32) % 2)[None, None, :]
    query_hit = jnp.repeat(own_hit, 2, axis=2) & (jnp.repeat(which_query, 2, axis=2) == head_parity)
    pattern_heads = jnp.repeat(pattern, 2, axis=2)
    scale_heads = jnp.repeat(scale_query, 2, axis=2)
    aligned = scale_heads[..., None] * pattern_heads
    values = jnp.where(query_hit[..., None], aligned, filler)
    return values.reshape(LENGTH, H * HD).astype(jnp.bfloat16)


def steps_of(key, extent, pieces, low, high):
    level = 1.0
    for axis_at, shards_of in pieces:
        draws = jax.random.uniform(jax.random.fold_in(jax.random.fold_in(key, 6), axis_at), (shards_of,), jnp.float32, low / len(pieces), high / len(pieces))
        level = level * jnp.repeat(jnp.exp(draws), extent[axis_at] // shards_of).reshape((-1,) + (1,) * (len(extent) - 1 - axis_at))
    return level


def length_profile(number_of, total, most, lean):
    portions = [(1 << 20) // math.isqrt(standing ** lean) + 1 for standing in range(2, number_of + 1)]
    spare, given = total - most - (number_of - 1), [1] * (number_of - 1)
    while spare > 0:
        free = [i for i in range(number_of - 1) if given[i] < most]
        pool, left = sum([portions[i] for i in free]), spare
        for i in free:
            more = min(most - given[i], max(1, left * portions[i] // pool), spare)
            given[i] = given[i] + more
            spare = spare - more
    return np.array([most] + given)


def ragged_sizes(own_key, number_of, total, most, lean):
    if number_of == 2:
        one = jax.random.randint(own_key, (), max(1, total - most), min(most, total - 1) + 1)
        return jnp.stack([one, total - one])
    tallies = jnp.asarray(length_profile(number_of, total, most, lean), jnp.int32)
    twos = (number_of - 1) // 2
    source_of, taker = tallies[1:1 + 2 * twos:2], tallies[2:2 + 2 * twos:2]
    room = jnp.minimum(source_of - 1, most - taker)
    moved = jax.random.randint(jax.random.fold_in(own_key, 1), (twos,), 0, 1 << 20) % (room + 1)
    tallies = tallies.at[1:1 + 2 * twos:2].set(source_of - moved).at[2:2 + 2 * twos:2].set(taker + moved)
    return tallies[jax.random.permutation(jax.random.fold_in(own_key, 2), number_of)]


def bell_draw(stream_key, dims, scale, reach, split=(), kind=jnp.bfloat16):
    array = jax.random.normal(stream_key, dims, jnp.float32) * scale
    if len(split) > 0:
        array = steps_of(stream_key, dims, split, -0.22, 0.18) * array
    return jnp.clip(array, min=-reach, max=reach).astype(kind)


def setup_inputs(seed: int = 0, part: int = 0) -> dict:
    seeds = jax.random.split(jax.random.key(seed), 11)
    part_keys = jax.random.split(jax.random.fold_in(seeds[10], part), 11)
    return {
        "residual": bell_draw(part_keys[0], (LENGTH, D), 1.0, 6.0, ((0, 256),)),
        "queries": draw_queries(jax.random.fold_in(jax.random.fold_in(seeds[10], part), 71), part),
        "key_heads": draw_key_heads(jax.random.fold_in(jax.random.fold_in(seeds[10], part), 71), part),
        "value_heads": bell_draw(part_keys[3], (LENGTH, KVH * HD), 1.0, 6.0, ((0, 16), (1, 16))),
        "doc_blocks": ragged_sizes(part_keys[4], DOCS, NBLK, MOST_BLK, 2).astype(jnp.int32),
        "out_weight": draw_out_weight(jax.random.fold_in(seeds[10], 71), part),
        "post_gain": jnp.clip(1.0 + 0.18 * jax.random.normal(seeds[6], (D,), jnp.float32), 0.1, 1.9),
        "ffn_gain": jnp.clip(1.0 + 0.18 * jax.random.normal(seeds[7], (D,), jnp.float32), 0.1, 1.9),
        "gate_weight": bell_draw(seeds[8], (D, FF), D ** -0.5, 0.09375, ((0, 16), (1, 16))),
        "up_weight": bell_draw(seeds[9], (D, FF), D ** -0.5, 0.09375, ((0, 16), (1, 16))),
    }


SOFT_CAP = 50.0
NORM_EPS = 1e-06
ROPE_BASE = 10000.0

def rope_angles(positions, head_size):
    halfway = head_size // 2
    frequency = ROPE_BASE ** (-(jnp.arange(halfway, dtype=jnp.float32) * 2.0) / head_size)
    angles = positions.astype(jnp.float32)[:, None] * frequency[None, :]
    return (jnp.cos(angles), jnp.sin(angles))

def rotate(heads_in, cosine, sine_value, head_size):
    rows_here = heads_in.shape[0]
    reshaped = heads_in.astype(jnp.float32).reshape(rows_here, -1, head_size)
    leading = reshaped[:, :, :head_size // 2]
    trailing = reshaped[:, :, head_size // 2:]
    cos_wide = cosine[:, None, :]
    sin_wide = sine_value[:, None, :]
    turned = jnp.concatenate([leading * cos_wide - trailing * sin_wide, trailing * cos_wide + leading * sin_wide], axis=2)
    return turned.reshape(rows_here, -1).astype(jnp.bfloat16)

def doc_of(positions, doc_blocks):
    doc_ends = jnp.cumsum(doc_blocks)
    passed = positions[:, None] // BLOCK >= doc_ends[None, :]
    return lax.optimization_barrier(jnp.sum(passed.astype(jnp.int32), axis=1)).astype(jnp.int32)

def rms_scale(values):
    return values * lax.rsqrt(lax.optimization_barrier(jnp.mean(values * values, axis=-1, keepdims=True)) + NORM_EPS)

def gelu_gate(gate_sum, up_sum):
    return (jax.nn.gelu(gate_sum, approximate=True) * up_sum).astype(jnp.bfloat16)

def attend(running, query_rows, query_pos, query_doc, key_rows, value_rows, key_pos, key_doc, score_scale):
    scores = lax.dot_general(query_rows, key_rows, (((1,), (1,)), ((), ())), preferred_element_type=jnp.float32) * score_scale
    capped = SOFT_CAP * jnp.tanh(scores / SOFT_CAP)
    visible = (key_pos[None, :] <= query_pos[:, None]) & (key_doc[None, :] == query_doc[:, None])
    weights = jnp.where(visible, jnp.exp(capped), 0.0).astype(jnp.bfloat16)
    numerator = running[0] + jnp.dot(weights, value_rows, preferred_element_type=jnp.float32)
    denominator = running[1] + lax.optimization_barrier(jnp.sum(weights.astype(jnp.float32), axis=1))
    return (numerator, denominator)

def reference(residual, queries, key_heads, value_heads, doc_blocks, out_weight, post_gain, ffn_gain, gate_weight, up_weight):
    length = residual.shape[0]
    positions = jnp.arange(length, dtype=jnp.int32)
    doc_ids = doc_of(positions, doc_blocks)
    cosine, sine_value = rope_angles(positions, HD)
    query_rot = rotate(queries, cosine, sine_value, HD).reshape(length, H, HD)
    key_rot = rotate(key_heads, cosine, sine_value, HD).reshape(length, KVH, HD)
    value_split = value_heads.reshape(length, KVH, HD)
    weight_split = out_weight.reshape(H, HD, D)
    score_scale = HD ** (-0.5)

    def one_head(summed, head_index):
        query_head = lax.dynamic_index_in_dim(query_rot, head_index, 1, keepdims=False)
        key_head = lax.dynamic_index_in_dim(key_rot, head_index // 2, 1, keepdims=False)
        value_head = lax.dynamic_index_in_dim(value_split, head_index // 2, 1, keepdims=False)

        def one_block(block_args):
            query_rows, query_pos, query_doc = block_args
            empty_sums = (jnp.zeros((TOK_CTX, HD), jnp.float32), jnp.zeros((TOK_CTX,), jnp.float32))
            numerator, denominator = attend(empty_sums, query_rows, query_pos, query_doc, key_head, value_head, positions, doc_ids, score_scale)
            return (numerator / denominator[:, None]).astype(jnp.bfloat16)
        attended = lax.map(one_block, (query_head.reshape(-1, TOK_CTX, HD), positions.reshape(-1, TOK_CTX), doc_ids.reshape(-1, TOK_CTX)))
        attended = attended.reshape(length, HD)
        head_weight = lax.dynamic_index_in_dim(weight_split, head_index, 0, keepdims=False)
        head_term = jnp.dot(attended, head_weight, preferred_element_type=jnp.float32).astype(jnp.bfloat16)
        head_term = lax.optimization_barrier(head_term)
        return (summed + head_term.astype(jnp.float32), None)
    attn_sum, _ = lax.scan(one_head, jnp.zeros((length, D), jnp.float32), jnp.arange(H, dtype=jnp.int32))
    mixed_stream = (residual.astype(jnp.float32) + rms_scale(attn_sum) * post_gain).astype(jnp.bfloat16)
    ffn_input = (rms_scale(mixed_stream.astype(jnp.float32)) * ffn_gain).astype(jnp.bfloat16)
    gate_sum = jnp.dot(ffn_input, gate_weight, preferred_element_type=jnp.float32)
    up_sum = jnp.dot(ffn_input, up_weight, preferred_element_type=jnp.float32)
    ffn_hidden = gelu_gate(gate_sum, up_sum)
    return (mixed_stream, ffn_hidden)
```

```python
import jax
import jax.numpy as jnp
from jax import lax
from jax.sharding import PartitionSpec as P

BLOCK = 32
MOST = 64 * BLOCK
SOFT_CAP = 50.0
NORM_EPS = 1e-06
ROPE_BASE = 10000.0
FAR = 4


def shift(value, axis, by):
    n = lax.axis_size(axis)
    return lax.ppermute(value, axis, [(i, (i + by) % n) for i in range(n)])


def rope_angles(positions, head_size):
    halfway = head_size // 2
    frequency = ROPE_BASE ** (-(jnp.arange(halfway, dtype=jnp.float32) * 2.0) / head_size)
    angles = positions.astype(jnp.float32)[:, None] * frequency[None, :]
    return (jnp.cos(angles), jnp.sin(angles))


def rotate(first, second, cosine, sine):
    first, second = (first.astype(jnp.float32), second.astype(jnp.float32))
    return jnp.concatenate(
        [first * cosine - second * sine, second * cosine + first * sine], axis=1
    ).astype(jnp.bfloat16)


def doc_of(positions, doc_blocks):
    doc_ends = jnp.cumsum(doc_blocks)
    passed = positions[:, None] // BLOCK >= doc_ends[None, :]
    return jnp.sum(passed.astype(jnp.int32), axis=1)


def rms_scale(values):
    return values * lax.rsqrt(jnp.mean(values * values, axis=-1, keepdims=True) + NORM_EPS)


def class_order(rows, t):
    by_class = jnp.moveaxis(rows.reshape(4, 4, 16, *rows.shape[1:]), 1, 0)
    return jnp.roll(by_class, -(t % 4), axis=0)


def per_device(
    residual,
    queries,
    key_heads,
    value_heads,
    doc_blocks,
    out_weight,
    post_gain,
    ffn_gain,
    gate_weight,
    up_weight,
):
    rows = queries.shape[0]
    hd = queries.shape[1]
    half = hd // 2
    c = lax.axis_index("ctx")
    t = lax.axis_index("tensor")
    n_ctx = lax.axis_size("ctx")
    stride4 = [[j + 4 * q for q in range(4)] for j in range(4)]

    weights = lax.all_gather(
        jnp.concatenate([gate_weight, up_weight], axis=1), "ctx", axis=0, tiled=True
    )

    partner = lax.ppermute(
        jnp.stack([key_heads, value_heads]), "tensor", [(i, i ^ 1) for i in range(16)]
    )
    own_first = t % 2 == 0
    pos = c * rows + jnp.arange(rows, dtype=jnp.int32)
    cosine, sine = rope_angles(pos, hd)
    k_lo = jnp.where(own_first, key_heads, partner[0])
    k_hi = jnp.where(own_first, partner[0], key_heads)
    v_lo = jnp.where(own_first, value_heads, partner[1])
    v_hi = jnp.where(own_first, partner[1], value_heads)
    block = jnp.concatenate([rotate(k_lo, k_hi, cosine, sine), v_lo, v_hi], axis=1)
    came = [
        lax.ppermute(block, "ctx", [(i, i + 2 * s) for i in range(n_ctx - 2 * s)])
        for s in range(FAR, 0, -1)
    ] + [block]
    mine = jnp.concatenate(came, axis=0)
    other = lax.ppermute(mine, "ctx", [(i, i ^ 1) for i in range(n_ctx)])
    chip = c // 2
    core = c % 2
    first_of = (chip - FAR + jnp.arange(FAR + 1, dtype=jnp.int32)) * 2
    inner = jnp.arange(rows, dtype=jnp.int32)
    pos_mine = ((first_of + core) * rows)[:, None] + inner[None, :]
    pos_other = ((first_of + 1 - core) * rows)[:, None] + inner[None, :]
    key_pos = jnp.concatenate([pos_mine.reshape(-1), pos_other.reshape(-1)])
    kv = jnp.concatenate([mine, other], axis=0)
    key_rows, value_rows = (kv[:, :hd], kv[:, hd:])

    q_pos = class_order(pos, t).reshape(4, 4, 2, 8)
    q_rot = rotate(queries[:, :half], queries[:, half:], cosine, sine)
    q_rot = class_order(q_rot, t).reshape(4, 4, 2, 8, hd)

    def leave(a):
        def g(r, h):
            return a[r, :, h].reshape(32, *a.shape[4:])
        return jnp.concatenate(
            [g(2, 0), g(1, 1), g(2, 1), g(3, 0), g(1, 0), g(3, 1), g(0, 0), g(0, 1)], axis=0
        )

    q_rows = leave(q_rot)
    q_pos = leave(q_pos)
    q_doc = doc_of(q_pos, doc_blocks)
    key_doc = doc_of(jnp.maximum(key_pos, 0), doc_blocks)
    scores = lax.dot_general(
        q_rows, key_rows, (((1,), (1,)), ((), ())), preferred_element_type=jnp.float32
    ) * (hd ** (-0.5))
    capped = SOFT_CAP * jnp.tanh(scores / SOFT_CAP)
    visible = (
        (key_pos[None, :] <= q_pos[:, None])
        & (key_doc[None, :] == q_doc[:, None])
        & (key_pos[None, :] >= 0)
    )
    probs = jnp.where(visible, jnp.exp(capped), 0.0).astype(jnp.bfloat16)
    numerator = jnp.dot(probs, value_rows, preferred_element_type=jnp.float32)
    denominator = jnp.sum(probs.astype(jnp.float32), axis=1)
    attended = (numerator / denominator[:, None]).astype(jnp.bfloat16)

    def out(a, b):
        return jnp.dot(
            attended[a:b], out_weight, preferred_element_type=jnp.float32
        ).astype(jnp.bfloat16)

    up_in = shift(out(0, 64), "tensor", 1)
    down_in = shift(out(64, 128), "tensor", -1)
    f32 = jnp.float32
    up_sum = (out(128, 160).astype(f32) + up_in[:32].astype(f32)).astype(jnp.bfloat16)
    up_two = shift(up_sum, "tensor", 1)
    down_sum = (out(160, 192).astype(f32) + down_in[:32].astype(f32)).astype(jnp.bfloat16)
    down_two = shift(down_sum, "tensor", -1)
    own = out(192, 256)
    sum_a = own[:32].astype(f32) + up_two.astype(f32) + down_in[32:].astype(f32)
    sum_b = own[32:].astype(f32) + up_in[32:].astype(f32) + down_two.astype(f32)
    d = residual.shape[1]
    sums = jnp.concatenate([sum_a.reshape(4, 8, d), sum_b.reshape(4, 8, d)], axis=1)
    parts = lax.all_to_all(
        sums.astype(jnp.bfloat16), "tensor", 0, 0, tiled=True, axis_index_groups=stride4
    )
    attn_rows = jnp.sum(parts.astype(f32), axis=0)

    mixed = (residual.astype(f32) + rms_scale(attn_rows) * post_gain).astype(jnp.bfloat16)
    ffn_in = (rms_scale(mixed.astype(f32)) * ffn_gain).astype(jnp.bfloat16)

    zero = lax.all_to_all(
        jnp.broadcast_to(ffn_in[None], (4, *ffn_in.shape)),
        "tensor",
        0,
        0,
        tiled=True,
        axis_index_groups=stride4,
    ).reshape(64, d)
    below = shift(zero, "tensor", 1)
    above = shift(zero, "tensor", -1)
    two_a = shift(below[:32], "tensor", 1)
    two_b = shift(above[32:], "tensor", -1)
    gathered = jnp.concatenate([zero, above, two_a, two_b, below], axis=0)
    ff = gate_weight.shape[1]
    gate_part = jnp.dot(gathered, weights[:, :ff], preferred_element_type=f32)
    up_part = jnp.dot(gathered, weights[:, ff:], preferred_element_type=f32)
    hidden = (jax.nn.gelu(gate_part, approximate=True) * up_part).astype(jnp.bfloat16)
    by_class = jnp.roll(hidden.reshape(4, 4, 16, ff), t % 4, axis=0)
    hidden = jnp.moveaxis(by_class, 0, 1).reshape(rows, ff)
    return (mixed, hidden)


def solution(mesh):
    in_specs = (
        P(("dp", "ctx", "tensor"), None),
        P(("dp", "ctx"), "tensor"),
        P(("dp", "ctx"), "tensor"),
        P(("dp", "ctx"), "tensor"),
        P("dp"),
        P("tensor", None),
        P(),
        P(),
        P("ctx", "tensor"),
        P("ctx", "tensor"),
    )
    out_specs = (P(("dp", "ctx", "tensor"), None), P(("dp", "ctx"), "tensor"))
    return jax.shard_map(
        per_device, mesh=mesh, in_specs=in_specs, out_specs=out_specs, check_vma=False
    )
```

```python
import jax
import jax.numpy as jnp
from jax import lax
from jax.sharding import PartitionSpec as P

BLOCK = 32
SOFT_CAP = 50.0
NORM_EPS = 1e-06
ROPE_BASE = 10000.0
FAR = 4
PIECE = 8


def swap(value, chain):
    n = lax.axis_size("tensor")
    ends = [(i, (i + 1) % n) for i in range(n) if i % 2 == chain]
    return lax.ppermute(value, "tensor", ends + [(j, i) for i, j in ends])


def rope_angles(positions, head_size):
    halfway = head_size // 2
    frequency = ROPE_BASE ** (-(jnp.arange(halfway, dtype=jnp.float32) * 2.0) / head_size)
    angles = positions.astype(jnp.float32)[:, None] * frequency[None, :]
    return (jnp.cos(angles), jnp.sin(angles))


def rotate(first, second, cosine, sine):
    first, second = (first.astype(jnp.float32), second.astype(jnp.float32))
    return jnp.concatenate(
        [first * cosine - second * sine, second * cosine + first * sine], axis=1
    ).astype(jnp.bfloat16)


def doc_of(positions, doc_blocks):
    doc_ends = jnp.cumsum(doc_blocks)
    passed = positions[:, None] // BLOCK >= doc_ends[None, :]
    return jnp.sum(passed.astype(jnp.int32), axis=1)


def rms_scale(values):
    return values * lax.rsqrt(jnp.mean(values * values, axis=-1, keepdims=True) + NORM_EPS)


def per_device(
    residual,
    queries,
    key_heads,
    value_heads,
    doc_blocks,
    out_weight,
    post_gain,
    ffn_gain,
    gate_weight,
    up_weight,
):
    f32 = jnp.float32
    bf16 = jnp.bfloat16
    rows = queries.shape[0]
    hd = queries.shape[1]
    d = residual.shape[1]
    ff = gate_weight.shape[1]
    half = hd // 2
    c = lax.axis_index("ctx")
    t = lax.axis_index("tensor")
    n_ctx = lax.axis_size("ctx")
    stride4 = [[j + 4 * q for q in range(4)] for j in range(4)]

    partner = swap(jnp.stack([key_heads, value_heads]), 0)
    weights = lax.all_gather(
        jnp.concatenate([gate_weight, up_weight], axis=1), "ctx", axis=0, tiled=True
    )
    own_first = t % 2 == 0
    pos = c * rows + jnp.arange(rows, dtype=jnp.int32)
    cosine, sine = rope_angles(pos, hd)
    k_lo = jnp.where(own_first, key_heads, partner[0])
    k_hi = jnp.where(own_first, partner[0], key_heads)
    v_lo = jnp.where(own_first, value_heads, partner[1])
    v_hi = jnp.where(own_first, partner[1], value_heads)
    block = jnp.concatenate([rotate(k_lo, k_hi, cosine, sine), v_lo, v_hi], axis=1)
    came = [
        lax.ppermute(block, "ctx", [(i, i + 2 * s) for i in range(n_ctx - 2 * s)])
        for s in range(FAR, 0, -1)
    ] + [block]
    mine = jnp.concatenate(came, axis=0)
    other = lax.ppermute(mine, "ctx", [(i, i ^ 1) for i in range(n_ctx)])
    chip = c // 2
    core = c % 2
    first_of = (chip - FAR + jnp.arange(FAR + 1, dtype=jnp.int32)) * 2
    inner = jnp.arange(rows, dtype=jnp.int32)
    pos_mine = ((first_of + core) * rows)[:, None] + inner[None, :]
    pos_other = ((first_of + 1 - core) * rows)[:, None] + inner[None, :]
    key_pos = jnp.concatenate([pos_mine.reshape(-1), pos_other.reshape(-1)])
    kv = jnp.concatenate([mine, other], axis=0)
    key_rows, value_rows = (kv[:, :hd], kv[:, hd:])

    way = [1 - 2 * ((t + chain) % 2) for chain in range(2)]

    def leave(a):
        a = a.reshape(4, 4, 2, PIECE, *a.shape[1:])

        def of(chain, r):
            one = lax.dynamic_index_in_dim(a[:, :, chain], (t + r) % 4, 1, keepdims=False)
            return one.reshape(4 * PIECE, *a.shape[4:])

        return jnp.concatenate(
            [of(x, r) for x in range(2) for r in (2, 4 + way[x])]
            + [of(x, r) for x in range(2) for r in (4 - way[x], 0)],
            axis=0,
        )

    q_rows = leave(rotate(queries[:, :half], queries[:, half:], cosine, sine))
    q_pos = leave(pos)
    q_doc = doc_of(q_pos, doc_blocks)
    key_doc = doc_of(jnp.maximum(key_pos, 0), doc_blocks)
    scores = lax.dot_general(
        q_rows, key_rows, (((1,), (1,)), ((), ())), preferred_element_type=f32
    ) * (hd ** (-0.5))
    capped = SOFT_CAP * jnp.tanh(scores / SOFT_CAP)
    visible = (
        (key_pos[None, :] <= q_pos[:, None])
        & (key_doc[None, :] == q_doc[:, None])
        & (key_pos[None, :] >= 0)
    )
    probs = jnp.where(visible, jnp.exp(capped), 0.0).astype(bf16)
    numerator = jnp.dot(probs, value_rows, preferred_element_type=f32)
    denominator = jnp.sum(probs.astype(f32), axis=1)
    attended = (numerator / denominator[:, None]).astype(bf16)

    def out(a):
        return jnp.dot(attended[a : a + 64], out_weight, preferred_element_type=f32).astype(bf16)

    sent = [swap(out(64 * x), x) for x in range(2)]
    kept = [out(128 + 64 * x) for x in range(2)]
    both = [kept[x].astype(f32) + sent[x].astype(f32) for x in range(2)]
    again = [swap(both[x][:32].astype(bf16), 1 - x) for x in range(2)]
    sums = [(both[x][32:] + again[x].astype(f32)).astype(bf16) for x in range(2)]

    def across(a):
        return lax.all_to_all(a, "tensor", 0, 0, tiled=True, axis_index_groups=stride4)

    parts = [across(sums[x].reshape(4, PIECE, d)) for x in range(2)]
    mixed, zero = ([], [])
    for x in range(2):
        attn_rows = jnp.sum(parts[x].astype(f32), axis=0)
        stream = residual[PIECE * x : PIECE * (x + 1)].astype(f32)
        stream = (stream + rms_scale(attn_rows) * post_gain).astype(bf16)
        ffn_in = (rms_scale(stream.astype(f32)) * ffn_gain).astype(bf16)
        mixed.append(stream)
        zero.append(across(jnp.broadcast_to(ffn_in[None], (4, PIECE, d))).reshape(32, d))
    one = [swap(zero[x], 1 - x) for x in range(2)]
    first = [jnp.concatenate([zero[x], one[x]], axis=0) for x in range(2)]
    second = [swap(first[x], x) for x in range(2)]
    gathered = jnp.concatenate([first[0], second[0], first[1], second[1]], axis=0)
    gate_part = jnp.dot(gathered, weights[:, :ff], preferred_element_type=f32)
    up_part = jnp.dot(gathered, weights[:, ff:], preferred_element_type=f32)
    hidden = (jax.nn.gelu(gate_part, approximate=True) * up_part).astype(bf16)

    hidden = hidden.reshape(2, 4, 4, PIECE, ff)

    def place(chain, j):
        r = (j - t) % 4
        at = jnp.where(r == 0, 0, jnp.where(r == 2, 3, jnp.where(r == (4 + way[chain]) % 4, 2, 1)))
        return lax.dynamic_index_in_dim(hidden[chain], at, 0, keepdims=False)

    hidden = jnp.stack(
        [jnp.stack([place(0, j), place(1, j)], axis=1) for j in range(4)], axis=1
    ).reshape(rows, ff)
    return (jnp.concatenate(mixed, axis=0), hidden)


def solution(mesh):
    in_specs = (
        P(("dp", "ctx", "tensor"), None),
        P(("dp", "ctx"), "tensor"),
        P(("dp", "ctx"), "tensor"),
        P(("dp", "ctx"), "tensor"),
        P("dp"),
        P("tensor", None),
        P(),
        P(),
        P("ctx", "tensor"),
        P("ctx", "tensor"),
    )
    out_specs = (P(("dp", "ctx", "tensor"), None), P(("dp", "ctx"), "tensor"))
    return jax.shard_map(
        per_device, mesh=mesh, in_specs=in_specs, out_specs=out_specs, check_vma=False
    )
```

```python
import jax
import jax.numpy as jnp
from jax import lax
from jax.experimental import pallas as pl
from jax.experimental.pallas import tpu as pltpu
from jax.sharding import PartitionSpec as P

BLOCK = 32
SOFT_CAP = 50.0
NORM_EPS = 1e-06
ROPE_BASE = 10000.0
FAR = 4
PIECE = 8


def swap(value, chain):
    n = lax.axis_size("tensor")
    ends = [(i, (i + 1) % n) for i in range(n) if i % 2 == chain]
    return lax.ppermute(value, "tensor", ends + [(j, i) for i, j in ends])


def rope_angles(positions, head_size):
    halfway = head_size // 2
    frequency = ROPE_BASE ** (-(jnp.arange(halfway, dtype=jnp.float32) * 2.0) / head_size)
    angles = positions.astype(jnp.float32)[:, None] * frequency[None, :]
    return (jnp.cos(angles), jnp.sin(angles))


def rotate(first, second, cosine, sine):
    first, second = (first.astype(jnp.float32), second.astype(jnp.float32))
    return jnp.concatenate(
        [first * cosine - second * sine, second * cosine + first * sine], axis=1
    ).astype(jnp.bfloat16)


def doc_of(positions, doc_blocks):
    doc_ends = jnp.cumsum(doc_blocks)
    passed = positions[:, None] // BLOCK >= doc_ends[None, :]
    return jnp.sum(passed.astype(jnp.int32), axis=1)


def rms_scale(values):
    return values * lax.rsqrt(jnp.mean(values * values, axis=-1, keepdims=True) + NORM_EPS)


def gated(total, ff):
    gate, up = (total[:, :ff], total[:, ff:])
    inner = 0.7978845608028654 * (gate + 0.044715 * gate * gate * gate)
    return (0.5 * gate * (1.0 + jnp.tanh(inner)) * up).astype(jnp.bfloat16)


def ffn_kernel(steps, ff, joined, parity_ref, *refs):
    pieces, (weight_ref, *rest) = (refs[:joined], refs[joined:])
    done_ref, out_ref, total = rest if len(rest) == 3 else (None, *rest)
    k = pl.program_id(0)
    a = jnp.concatenate([p[...] for p in pieces], axis=0) if joined > 1 else pieces[0][...]
    product = jnp.dot(a, weight_ref[...], preferred_element_type=jnp.float32)

    @pl.when(k == 0)
    def _():
        total[...] = product

    @pl.when(k > 0)
    def _():
        total[...] += product

    @pl.when(k == steps - 1)
    def _():
        hidden = gated(total[...], ff)
        if done_ref is None:
            out_ref[...] = hidden
        else:
            parity = parity_ref[0]
            out_ref[:, parity] = done_ref[...].reshape(8, 16, ff)
            out_ref[:, 1 - parity] = hidden.reshape(8, 16, ff)


def ffn(parity, pieces, weights, done):
    depth, width = weights.shape
    ff = width // 2
    rows = sum(p.shape[0] for p in pieces)
    step = 512
    steps = depth // step
    whole = [] if done is None else [done]
    shape = (rows, ff) if done is None else (8, 2, 16, ff)
    return pl.pallas_call(
        lambda *refs: ffn_kernel(steps, ff, len(pieces), *refs),
        out_shape=jax.ShapeDtypeStruct(shape, jnp.bfloat16),
        grid=(steps,),
        in_specs=[pl.BlockSpec(memory_space=pltpu.SMEM)]
        + [pl.BlockSpec((p.shape[0], step), lambda k: (0, k)) for p in pieces]
        + [pl.BlockSpec((step, width), lambda k: (k, 0))]
        + [pl.BlockSpec((rows, ff), lambda k: (0, 0)) for _ in whole],
        out_specs=pl.BlockSpec(shape, lambda k: (0,) * len(shape)),
        scratch_shapes=[pltpu.VMEM((rows, width), jnp.float32)],
        cost_estimate=pl.CostEstimate(
            flops=2 * rows * depth * width,
            bytes_accessed=2 * depth * width,
            transcendentals=rows * ff,
        ),
        name="ffn",
    )(parity, *pieces, weights, *whole)


def per_device(
    residual,
    queries,
    key_heads,
    value_heads,
    doc_blocks,
    out_weight,
    post_gain,
    ffn_gain,
    gate_weight,
    up_weight,
):
    f32 = jnp.float32
    bf16 = jnp.bfloat16
    rows = queries.shape[0]
    hd = queries.shape[1]
    d = residual.shape[1]
    ff = gate_weight.shape[1]
    half = hd // 2
    c = lax.axis_index("ctx")
    t = lax.axis_index("tensor")
    n_ctx = lax.axis_size("ctx")
    stride4 = [[j + 4 * q for q in range(4)] for j in range(4)]

    partner = swap(jnp.stack([key_heads, value_heads]), 0)
    partner, gate_weight, up_weight = lax.optimization_barrier((partner, gate_weight, up_weight))
    weights = lax.all_gather(
        jnp.concatenate([gate_weight, up_weight], axis=1), "ctx", axis=0, tiled=True
    )
    own_first = t % 2 == 0
    pos = c * rows + jnp.arange(rows, dtype=jnp.int32)
    cosine, sine = rope_angles(pos, hd)
    k_lo = jnp.where(own_first, key_heads, partner[0])
    k_hi = jnp.where(own_first, partner[0], key_heads)
    v_lo = jnp.where(own_first, value_heads, partner[1])
    v_hi = jnp.where(own_first, partner[1], value_heads)
    block = jnp.concatenate([rotate(k_lo, k_hi, cosine, sine), v_lo, v_hi], axis=1)
    came = [
        lax.ppermute(block, "ctx", [(i, i + 2 * s) for i in range(n_ctx - 2 * s)])
        for s in range(FAR, 0, -1)
    ] + [block]
    mine = jnp.concatenate(came, axis=0)
    other = lax.ppermute(mine, "ctx", [(i, i ^ 1) for i in range(n_ctx)])
    chip = c // 2
    core = c % 2
    first_of = (chip - FAR + jnp.arange(FAR + 1, dtype=jnp.int32)) * 2
    inner = jnp.arange(rows, dtype=jnp.int32)
    pos_mine = ((first_of + core) * rows)[:, None] + inner[None, :]
    pos_other = ((first_of + 1 - core) * rows)[:, None] + inner[None, :]
    key_pos = jnp.concatenate([pos_mine.reshape(-1), pos_other.reshape(-1)])
    kv = jnp.concatenate([mine, other], axis=0)
    key_rows, value_rows = (kv[:, :hd], kv[:, hd:])

    way = [1 - 2 * ((t + chain) % 2) for chain in range(2)]

    def leave(a):
        a = a.reshape(4, 4, 2, PIECE, *a.shape[1:])

        def of(chain, r):
            one = lax.dynamic_index_in_dim(a[:, :, chain], (t + r) % 4, 1, keepdims=False)
            return one.reshape(4 * PIECE, *a.shape[4:])

        return jnp.concatenate(
            [of(x, r) for x in range(2) for r in (2, 4 + way[x])]
            + [of(x, r) for x in range(2) for r in (4 - way[x], 0)],
            axis=0,
        )

    q_rows = leave(rotate(queries[:, :half], queries[:, half:], cosine, sine))
    q_pos = leave(pos)
    q_doc = doc_of(q_pos, doc_blocks)
    key_doc = doc_of(jnp.maximum(key_pos, 0), doc_blocks)
    scores = lax.dot_general(
        q_rows, key_rows, (((1,), (1,)), ((), ())), preferred_element_type=f32
    ) * (hd ** (-0.5))
    capped = SOFT_CAP * jnp.tanh(scores / SOFT_CAP)
    visible = (
        (key_pos[None, :] <= q_pos[:, None])
        & (key_doc[None, :] == q_doc[:, None])
        & (key_pos[None, :] >= 0)
    )
    probs = jnp.where(visible, jnp.exp(capped), 0.0).astype(bf16)
    numerator = jnp.dot(probs, value_rows, preferred_element_type=f32)
    denominator = jnp.sum(probs.astype(f32), axis=1)
    attended = (numerator / denominator[:, None]).astype(bf16)

    def out(a):
        return jnp.dot(attended[a : a + 64], out_weight, preferred_element_type=f32).astype(bf16)

    sent = [swap(out(64 * x), x) for x in range(2)]
    kept = [out(128 + 64 * x) for x in range(2)]
    both = [kept[x].astype(f32) + sent[x].astype(f32) for x in range(2)]
    again = [swap(both[x][:32].astype(bf16), 1 - x) for x in range(2)]
    sums = [(both[x][32:] + again[x].astype(f32)).astype(bf16) for x in range(2)]

    sums = jnp.stack([a.reshape(4, PIECE, d) for a in sums], axis=1).reshape(4, 2 * PIECE, d)
    parts = lax.all_to_all(sums, "tensor", 0, 0, tiled=True, axis_index_groups=stride4)
    attn_rows = jnp.sum(parts.astype(f32), axis=0)
    mixed = (residual.astype(f32) + rms_scale(attn_rows) * post_gain).astype(bf16)
    ffn_in = (rms_scale(mixed.astype(f32)) * ffn_gain).astype(bf16)

    stride2 = [[j + 2 * m for m in range(8)] for j in range(2)]
    own = lax.all_gather(ffn_in, "tensor", axis=0, tiled=True, axis_index_groups=stride2)
    own, weights = lax.optimization_barrier((own, weights))
    rest = [swap(own[64 * x : 64 * (x + 1)], x) for x in range(2)]
    parity = (t % 2).astype(jnp.int32).reshape(1)
    done = ffn(parity, [own], weights, None)
    hidden = ffn(parity, rest, weights, done)
    return (mixed, hidden.reshape(rows, ff))


def solution(mesh):
    in_specs = (
        P(("dp", "ctx", "tensor"), None),
        P(("dp", "ctx"), "tensor"),
        P(("dp", "ctx"), "tensor"),
        P(("dp", "ctx"), "tensor"),
        P("dp"),
        P("tensor", None),
        P(),
        P(),
        P("ctx", "tensor"),
        P("ctx", "tensor"),
    )
    out_specs = (P(("dp", "ctx", "tensor"), None), P(("dp", "ctx"), "tensor"))
    return jax.shard_map(
        per_device, mesh=mesh, in_specs=in_specs, out_specs=out_specs, check_vma=False
    )
```

```python
import jax
import jax.numpy as jnp
from jax import lax
from jax.experimental import pallas as pl
from jax.experimental.pallas import tpu as pltpu
from jax.sharding import PartitionSpec as P

BLOCK = 32
SOFT_CAP = 50.0
NORM_EPS = 1e-06
ROPE_BASE = 10000.0
FAR = 4


def twin(v):
    return v ^ (v >> 3)


def swap(value, chain):
    n = lax.axis_size("tensor")
    ends = [(i, (i + 1) % n) for i in range(n) if i % 2 == chain]
    return lax.ppermute(value, "tensor", ends + [(j, i) for i, j in ends])


def swap_pairs(value, chain):
    n = lax.axis_size("tensor")
    ends = [(twin(v), twin((v + 2) % n)) for v in range(n) if (v // 2) % 2 == chain]
    return lax.ppermute(value, "tensor", ends + [(j, i) for i, j in ends])


def rope_angles(positions, head_size):
    halfway = head_size // 2
    frequency = ROPE_BASE ** (-(jnp.arange(halfway, dtype=jnp.float32) * 2.0) / head_size)
    angles = positions.astype(jnp.float32)[:, None] * frequency[None, :]
    return (jnp.cos(angles), jnp.sin(angles))


def rotate(first, second, cosine, sine):
    first, second = (first.astype(jnp.float32), second.astype(jnp.float32))
    return jnp.concatenate(
        [first * cosine - second * sine, second * cosine + first * sine], axis=1
    ).astype(jnp.bfloat16)


def doc_of(positions, doc_blocks):
    doc_ends = jnp.cumsum(doc_blocks)
    passed = positions[:, None] // BLOCK >= doc_ends[None, :]
    return jnp.sum(passed.astype(jnp.int32), axis=1)


def rms_scale(values):
    return values * lax.rsqrt(jnp.mean(values * values, axis=-1, keepdims=True) + NORM_EPS)


def gated(total, ff):
    gate, up = (total[:, :ff], total[:, ff:])
    inner = 0.7978845608028654 * (gate + 0.044715 * gate * gate * gate)
    return (0.5 * gate * (1.0 + jnp.tanh(inner)) * up).astype(jnp.bfloat16)


def ffn_kernel(steps, ff, joined, parity_ref, *refs):
    pieces, (weight_ref, *rest) = (refs[:joined], refs[joined:])
    done_ref, out_ref, total = rest if len(rest) == 3 else (None, *rest)
    k = pl.program_id(0)
    a = jnp.concatenate([p[...] for p in pieces], axis=0) if joined > 1 else pieces[0][...]
    product = jnp.dot(a, weight_ref[...], preferred_element_type=jnp.float32)

    @pl.when(k == 0)
    def _():
        total[...] = product

    @pl.when(k > 0)
    def _():
        total[...] += product

    @pl.when(k == steps - 1)
    def _():
        hidden = gated(total[...], ff)
        if done_ref is None:
            out_ref[...] = hidden
        else:
            parity = parity_ref[0]
            out_ref[:, parity] = done_ref[...].reshape(8, 16, ff)
            out_ref[:, 1 - parity] = hidden.reshape(8, 16, ff)


def ffn(parity, pieces, weights, done):
    depth, width = weights.shape
    ff = width // 2
    rows = sum(p.shape[0] for p in pieces)
    step = 896
    steps = depth // step
    whole = [] if done is None else [done]
    shape = (rows, ff) if done is None else (8, 2, 16, ff)
    return pl.pallas_call(
        lambda *refs: ffn_kernel(steps, ff, len(pieces), *refs),
        out_shape=jax.ShapeDtypeStruct(shape, jnp.bfloat16),
        grid=(steps,),
        in_specs=[pl.BlockSpec(memory_space=pltpu.SMEM)]
        + [pl.BlockSpec((p.shape[0], step), lambda k: (0, k)) for p in pieces]
        + [pl.BlockSpec((step, width), lambda k: (k, 0))]
        + [pl.BlockSpec((rows, ff), lambda k: (0, 0)) for _ in whole],
        out_specs=pl.BlockSpec(shape, lambda k: (0,) * len(shape)),
        scratch_shapes=[pltpu.VMEM((rows, width), jnp.float32)],
        cost_estimate=pl.CostEstimate(
            flops=2 * rows * depth * width,
            bytes_accessed=2 * depth * width,
            transcendentals=rows * ff,
        ),
        name="ffn",
    )(parity, *pieces, weights, *whole)


def per_device(
    residual,
    queries,
    key_heads,
    value_heads,
    doc_blocks,
    out_weight,
    post_gain,
    ffn_gain,
    gate_weight,
    up_weight,
):
    f32 = jnp.float32
    bf16 = jnp.bfloat16
    rows = queries.shape[0]
    hd = queries.shape[1]
    d = residual.shape[1]
    ff = gate_weight.shape[1]
    half = hd // 2
    c = lax.axis_index("ctx")
    t = lax.axis_index("tensor")
    n_ctx = lax.axis_size("ctx")
    far = [[twin(4 * q + j) for q in range(4)] for j in range(4)]
    v = twin(t)

    chunks = queries.reshape(8, 2, 16, hd)
    first_goes = (jnp.arange(8, dtype=jnp.int32) // 4 != v % 2)[:, None, None]
    q_send = jnp.where(first_goes, chunks[:, 0], chunks[:, 1]).reshape(rows // 2, hd)
    q_keep = jnp.where(first_goes, chunks[:, 1], chunks[:, 0]).reshape(rows // 2, hd)
    q_send = jnp.concatenate([q_send[:, :half], q_send[:, half:]], axis=0)
    partner = swap(jnp.stack([key_heads, value_heads]), 0)
    weights = jnp.concatenate([gate_weight, up_weight], axis=1)
    weights = lax.all_gather(weights, "ctx", axis=0, tiled=True)
    core = c % 2
    weight_half = lax.dynamic_slice_in_dim(out_weight, core * half, half, axis=0)
    weight_half = swap(weight_half, 0)
    q_came = swap(q_send, 0)

    own_first = t % 2 == 0
    pos = c * rows + jnp.arange(rows, dtype=jnp.int32)
    cosine, sine = rope_angles(pos, hd)
    k_lo = jnp.where(own_first, key_heads, partner[0])
    k_hi = jnp.where(own_first, partner[0], key_heads)
    v_lo = jnp.where(own_first, value_heads, partner[1])
    v_hi = jnp.where(own_first, partner[1], value_heads)
    block = jnp.concatenate([rotate(k_lo, k_hi, cosine, sine), v_lo, v_hi], axis=1)
    came = [
        lax.ppermute(block, "ctx", [(i, i + 2 * s) for i in range(n_ctx - 2 * s)])
        for s in range(FAR, 0, -1)
    ]
    mine = jnp.concatenate(came + [block], axis=0)
    both_cores = [(i, i ^ 1) for i in range(n_ctx)]
    other = lax.ppermute(mine, "ctx", both_cores)
    weight_rest = lax.ppermute(weight_half, "ctx", both_cores)
    partner_weight = jnp.concatenate([weight_half, weight_rest], axis=0)
    chip = c // 2
    first_of = (chip - FAR + jnp.arange(FAR + 1, dtype=jnp.int32)) * 2
    inner = jnp.arange(rows, dtype=jnp.int32)
    pos_mine = ((first_of + core) * rows)[:, None] + inner[None, :]
    pos_other = ((first_of + 1 - core) * rows)[:, None] + inner[None, :]
    key_pos = jnp.concatenate([pos_mine.reshape(-1), pos_other.reshape(-1)])
    kv = jnp.concatenate([mine, other], axis=0)
    key_rows, value_rows = (kv[:, :hd], kv[:, hd:])

    upper = (v // 2) % 2 == 1

    def by_class(a):
        a = a.reshape(4, 2, 16, *a.shape[1:])
        leave = jnp.where(upper, a[:, 0], a[:, 1])
        stay = jnp.where(upper, a[:, 1], a[:, 0])
        return jnp.concatenate([leave, stay], axis=0).reshape(rows // 2, *a.shape[3:])

    w = 2 * jnp.arange(8, dtype=jnp.int32) + v % 2
    share_pos = by_class(
        (c * rows + twin(w)[:, None] * 16 + jnp.arange(16, dtype=jnp.int32)[None, :]).reshape(-1)
    )
    q_cos, q_sin = rope_angles(share_pos, hd)

    def turned(lo, hi):
        return rotate(by_class(lo), by_class(hi), q_cos, q_sin)

    q_rows = jnp.concatenate(
        [
            turned(q_keep[:, :half], q_keep[:, half:]),
            turned(q_came[: rows // 2], q_came[rows // 2 :]),
        ],
        axis=0,
    )
    q_pos = jnp.concatenate([share_pos, share_pos])
    q_doc = doc_of(q_pos, doc_blocks)
    key_doc = doc_of(jnp.maximum(key_pos, 0), doc_blocks)
    scores = lax.dot_general(
        q_rows, key_rows, (((1,), (1,)), ((), ())), preferred_element_type=f32
    ) * (hd ** (-0.5))
    capped = SOFT_CAP * jnp.tanh(scores / SOFT_CAP)
    visible = (
        (key_pos[None, :] <= q_pos[:, None])
        & (key_doc[None, :] == q_doc[:, None])
        & (key_pos[None, :] >= 0)
    )
    probs = jnp.where(visible, jnp.exp(capped), 0.0).astype(bf16)
    numerator = jnp.dot(probs, value_rows, preferred_element_type=f32)
    denominator = jnp.sum(probs.astype(f32), axis=1)
    attended = (numerator / denominator[:, None]).astype(bf16)
    beside = attended[rows // 2 :]
    turned_round = jnp.concatenate([beside[:, half:], beside[:, :half]], axis=1)
    both_heads = (attended[: rows // 2], jnp.where(core == 0, beside, turned_round))

    def out(a):
        return jnp.dot(
            both_heads[0][a : a + 64], out_weight, preferred_element_type=f32
        ) + jnp.dot(both_heads[1][a : a + 64], partner_weight, preferred_element_type=f32)

    leaves = out(0).astype(bf16)
    sent = [swap_pairs(leaves[32 * x : 32 * (x + 1)], x) for x in range(2)]
    sums = out(64) + jnp.concatenate(sent, axis=0).astype(f32)
    parts = lax.all_to_all(
        sums.astype(bf16).reshape(4, 16, d), "tensor", 0, 0, tiled=True, axis_index_groups=far
    )
    attn_rows = jnp.sum(parts.astype(f32), axis=0)
    mixed = (residual.astype(f32) + rms_scale(attn_rows) * post_gain).astype(bf16)
    ffn_in = (rms_scale(mixed.astype(f32)) * ffn_gain).astype(bf16)

    stride2 = [[j + 2 * m for m in range(8)] for j in range(2)]
    own = lax.all_gather(ffn_in, "tensor", axis=0, tiled=True, axis_index_groups=stride2)
    own, weights = lax.optimization_barrier((own, weights))
    rest = [swap(own[64 * x : 64 * (x + 1)], x) for x in range(2)]
    parity = (t % 2).astype(jnp.int32).reshape(1)
    done = ffn(parity, [own], weights, None)
    hidden = ffn(parity, rest, weights, done)
    return (mixed, hidden.reshape(rows, ff))


def solution(mesh):
    in_specs = (
        P(("dp", "ctx", "tensor"), None),
        P(("dp", "ctx"), "tensor"),
        P(("dp", "ctx"), "tensor"),
        P(("dp", "ctx"), "tensor"),
        P("dp"),
        P("tensor", None),
        P(),
        P(),
        P("ctx", "tensor"),
        P("ctx", "tensor"),
    )
    out_specs = (P(("dp", "ctx", "tensor"), None), P(("dp", "ctx"), "tensor"))
    return jax.shard_map(
        per_device, mesh=mesh, in_specs=in_specs, out_specs=out_specs, check_vma=False
    )
```

```python
import jax
import jax.numpy as jnp
from jax import lax
from jax.experimental import pallas as pl
from jax.experimental.pallas import tpu as pltpu
from jax.sharding import PartitionSpec as P

BLOCK = 32
SOFT_CAP = 50.0
NORM_EPS = 1e-06
ROPE_BASE = 10000.0
FAR = 4


def twin(v):
    return v ^ (v >> 3)


def swap(value, chain):
    n = lax.axis_size("tensor")
    ends = [(i, (i + 1) % n) for i in range(n) if i % 2 == chain]
    return lax.ppermute(value, "tensor", ends + [(j, i) for i, j in ends])


def swap_pairs(value, chain):
    n = lax.axis_size("tensor")
    ends = [(twin(v), twin((v + 2) % n)) for v in range(n) if (v // 2) % 2 == chain]
    return lax.ppermute(value, "tensor", ends + [(j, i) for i, j in ends])


def rope_angles(positions, head_size):
    halfway = head_size // 2
    frequency = ROPE_BASE ** (-(jnp.arange(halfway, dtype=jnp.float32) * 2.0) / head_size)
    angles = positions.astype(jnp.float32)[:, None] * frequency[None, :]
    return (jnp.cos(angles), jnp.sin(angles))


def rotate(first, second, cosine, sine):
    first, second = (first.astype(jnp.float32), second.astype(jnp.float32))
    return jnp.concatenate(
        [first * cosine - second * sine, second * cosine + first * sine], axis=1
    ).astype(jnp.bfloat16)


def doc_of(positions, doc_blocks):
    doc_ends = jnp.cumsum(doc_blocks)
    passed = positions[:, None] // BLOCK >= doc_ends[None, :]
    return jnp.sum(passed.astype(jnp.int32), axis=1)


def rms_scale(values):
    return values * lax.rsqrt(jnp.mean(values * values, axis=-1, keepdims=True) + NORM_EPS)


def gated(total, ff):
    gate, up = (total[:, :ff], total[:, ff:])
    inner = 0.7978845608028654 * (gate + 0.044715 * gate * gate * gate)
    return (0.5 * gate * (1.0 + jnp.tanh(inner)) * up).astype(jnp.bfloat16)


STEP = 896


def add_up(pieces, weight_ref, wait):
    total = None
    for at in range(0, weight_ref.shape[0], STEP):
        wait(at)
        a = [p[:, at : at + STEP] for p in pieces]
        a = jnp.concatenate(a, axis=0) if len(a) > 1 else a[0]
        product = jnp.dot(a, weight_ref[at : at + STEP], preferred_element_type=jnp.float32)
        total = product if total is None else total + product
    return gated(total, weight_ref.shape[1] // 2)


def own_kernel(a_ref, weight_ref, out_ref, kept_ref, sems):
    copies = {
        at: pltpu.make_async_copy(
            weight_ref.at[pl.ds(at, STEP)], kept_ref.at[pl.ds(at, STEP)], sems.at[at // STEP]
        )
        for at in range(0, weight_ref.shape[0], STEP)
    }
    for copy in copies.values():
        copy.start()
    out_ref[...] = add_up([a_ref], kept_ref, lambda at: copies[at].wait())


def rest_kernel(parity_ref, a_ref, b_ref, weight_ref, done_ref, out_ref):
    hidden = add_up([a_ref, b_ref], weight_ref, lambda at: None)
    parity = parity_ref[0]
    shape = (8, 16, hidden.shape[1])
    out_ref[:, parity] = done_ref[...].reshape(shape)
    out_ref[:, 1 - parity] = hidden.reshape(shape)


def cost(rows, weights):
    depth, width = weights.shape
    return pl.CostEstimate(
        flops=2 * rows * depth * width,
        bytes_accessed=2 * depth * width,
        transcendentals=rows * width // 2,
    )


def ffn_own(own, weights):
    rows, ff = (own.shape[0], weights.shape[1] // 2)
    in_vmem = pl.BlockSpec(memory_space=pltpu.VMEM)
    return pl.pallas_call(
        own_kernel,
        out_shape=(
            jax.ShapeDtypeStruct((rows, ff), jnp.bfloat16),
            pltpu.VMEM(weights.shape, jnp.bfloat16),
        ),
        in_specs=[in_vmem, pl.BlockSpec(memory_space=pl.ANY)],
        out_specs=(in_vmem, in_vmem),
        scratch_shapes=[pltpu.SemaphoreType.DMA((weights.shape[0] // STEP,))],
        cost_estimate=cost(rows, weights),
        compiler_params=pltpu.CompilerParams(vmem_limit_bytes=42 * 2**20),
        name="ffn_own",
    )(own, weights)


def ffn_rest(parity, pieces, weights, done):
    ff = weights.shape[1] // 2
    in_vmem = pl.BlockSpec(memory_space=pltpu.VMEM)
    return pl.pallas_call(
        rest_kernel,
        out_shape=jax.ShapeDtypeStruct((8, 2, 16, ff), jnp.bfloat16),
        in_specs=[pl.BlockSpec(memory_space=pltpu.SMEM)] + [in_vmem] * 4,
        out_specs=in_vmem,
        cost_estimate=cost(done.shape[0], weights),
        compiler_params=pltpu.CompilerParams(vmem_limit_bytes=24 * 2**20),
        name="ffn_rest",
    )(parity, *pieces, weights, done)


def per_device(
    residual,
    queries,
    key_heads,
    value_heads,
    doc_blocks,
    out_weight,
    post_gain,
    ffn_gain,
    gate_weight,
    up_weight,
):
    f32 = jnp.float32
    bf16 = jnp.bfloat16
    rows = queries.shape[0]
    hd = queries.shape[1]
    d = residual.shape[1]
    ff = gate_weight.shape[1]
    half = hd // 2
    c = lax.axis_index("ctx")
    t = lax.axis_index("tensor")
    n_ctx = lax.axis_size("ctx")
    far = [[twin(4 * q + j) for q in range(4)] for j in range(4)]
    v = twin(t)

    chunks = queries.reshape(8, 2, 16, hd)
    first_goes = (jnp.arange(8, dtype=jnp.int32) // 4 != v % 2)[:, None, None]
    q_send = jnp.where(first_goes, chunks[:, 0], chunks[:, 1]).reshape(rows // 2, hd)
    q_keep = jnp.where(first_goes, chunks[:, 1], chunks[:, 0]).reshape(rows // 2, hd)
    q_send = jnp.concatenate([q_send[:, :half], q_send[:, half:]], axis=0)
    partner = swap(jnp.stack([key_heads, value_heads]), 0)
    weights = jnp.concatenate([gate_weight, up_weight], axis=1)
    weights = lax.all_gather(weights, "ctx", axis=0, tiled=True)
    core = c % 2
    weight_half = lax.dynamic_slice_in_dim(out_weight, core * half, half, axis=0)
    weight_half = swap(weight_half, 0)
    q_came = swap(q_send, 0)

    own_first = t % 2 == 0
    pos = c * rows + jnp.arange(rows, dtype=jnp.int32)
    cosine, sine = rope_angles(pos, hd)
    k_lo = jnp.where(own_first, key_heads, partner[0])
    k_hi = jnp.where(own_first, partner[0], key_heads)
    v_lo = jnp.where(own_first, value_heads, partner[1])
    v_hi = jnp.where(own_first, partner[1], value_heads)
    block = jnp.concatenate([rotate(k_lo, k_hi, cosine, sine), v_lo, v_hi], axis=1)

    def ahead(by):
        return lax.ppermute(block, "ctx", [(i, i + 2 * by) for i in range(n_ctx - 2 * by)])

    came = [ahead(FAR)]
    came = came + [ahead(by) for by in range(FAR - 1, 0, -1)]
    mine = jnp.concatenate(came + [block], axis=0)
    both_cores = [(i, i ^ 1) for i in range(n_ctx)]
    other = lax.ppermute(mine, "ctx", both_cores)
    weight_rest = lax.ppermute(weight_half, "ctx", both_cores)
    partner_weight = jnp.concatenate([weight_half, weight_rest], axis=0)
    chip = c // 2
    first_of = (chip - FAR + jnp.arange(FAR + 1, dtype=jnp.int32)) * 2
    inner = jnp.arange(rows, dtype=jnp.int32)
    pos_mine = ((first_of + core) * rows)[:, None] + inner[None, :]
    pos_other = ((first_of + 1 - core) * rows)[:, None] + inner[None, :]
    key_pos = jnp.concatenate([pos_mine.reshape(-1), pos_other.reshape(-1)])
    kv = jnp.concatenate([mine, other], axis=0)
    key_rows, value_rows = (kv[:, :hd], kv[:, hd:])

    upper = (v // 2) % 2 == 1

    def by_class(a):
        a = a.reshape(4, 2, 16, *a.shape[1:])
        leave = jnp.where(upper, a[:, 0], a[:, 1])
        stay = jnp.where(upper, a[:, 1], a[:, 0])
        return jnp.concatenate([leave, stay], axis=0).reshape(rows // 2, *a.shape[3:])

    w = 2 * jnp.arange(8, dtype=jnp.int32) + v % 2
    share_pos = by_class(
        (c * rows + twin(w)[:, None] * 16 + jnp.arange(16, dtype=jnp.int32)[None, :]).reshape(-1)
    )
    q_cos, q_sin = rope_angles(share_pos, hd)

    def turned(lo, hi):
        return rotate(by_class(lo), by_class(hi), q_cos, q_sin)

    q_rows = jnp.concatenate(
        [
            turned(q_keep[:, :half], q_keep[:, half:]),
            turned(q_came[: rows // 2], q_came[rows // 2 :]),
        ],
        axis=0,
    )
    q_pos = jnp.concatenate([share_pos, share_pos])
    q_doc = doc_of(q_pos, doc_blocks)
    key_doc = doc_of(jnp.maximum(key_pos, 0), doc_blocks)
    scores = lax.dot_general(
        q_rows, key_rows, (((1,), (1,)), ((), ())), preferred_element_type=f32
    ) * (hd ** (-0.5))
    capped = SOFT_CAP * jnp.tanh(scores / SOFT_CAP)
    visible = (
        (key_pos[None, :] <= q_pos[:, None])
        & (key_doc[None, :] == q_doc[:, None])
        & (key_pos[None, :] >= 0)
    )
    probs = jnp.where(visible, jnp.exp(capped), 0.0).astype(bf16)
    numerator = jnp.dot(probs, value_rows, preferred_element_type=f32)
    denominator = jnp.sum(probs.astype(f32), axis=1)
    attended = (numerator / denominator[:, None]).astype(bf16)
    beside = attended[rows // 2 :]
    turned_round = jnp.concatenate([beside[:, half:], beside[:, :half]], axis=1)
    both_heads = (attended[: rows // 2], jnp.where(core == 0, beside, turned_round))

    def out(a):
        return jnp.dot(
            both_heads[0][a : a + 64], out_weight, preferred_element_type=f32
        ) + jnp.dot(both_heads[1][a : a + 64], partner_weight, preferred_element_type=f32)

    leaves = out(0).astype(bf16)
    sent = [swap_pairs(leaves[32 * x : 32 * (x + 1)], x) for x in range(2)]
    sums = out(64) + jnp.concatenate(sent, axis=0).astype(f32)
    parts = lax.all_to_all(
        sums.astype(bf16).reshape(4, 16, d), "tensor", 0, 0, tiled=True, axis_index_groups=far
    )
    attn_rows = jnp.sum(parts.astype(f32), axis=0)
    mixed = (residual.astype(f32) + rms_scale(attn_rows) * post_gain).astype(bf16)
    ffn_in = (rms_scale(mixed.astype(f32)) * ffn_gain).astype(bf16)

    stride2 = [[j + 2 * m for m in range(8)] for j in range(2)]
    own = lax.all_gather(ffn_in, "tensor", axis=0, tiled=True, axis_index_groups=stride2)
    own, weights = lax.optimization_barrier((own, weights))
    rest = [swap(own[64 * x : 64 * (x + 1)], x) for x in range(2)]
    parity = (t % 2).astype(jnp.int32).reshape(1)
    done, weights = ffn_own(own, weights)
    hidden = ffn_rest(parity, rest, weights, done)
    return (mixed, hidden.reshape(rows, ff))


def solution(mesh):
    in_specs = (
        P(("dp", "ctx", "tensor"), None),
        P(("dp", "ctx"), "tensor"),
        P(("dp", "ctx"), "tensor"),
        P(("dp", "ctx"), "tensor"),
        P("dp"),
        P("tensor", None),
        P(),
        P(),
        P("ctx", "tensor"),
        P("ctx", "tensor"),
    )
    out_specs = (P(("dp", "ctx", "tensor"), None), P(("dp", "ctx"), "tensor"))
    return jax.shard_map(
        per_device, mesh=mesh, in_specs=in_specs, out_specs=out_specs, check_vma=False
    )
```
